32 devices in a mesh: gx: 2 (over y), gy: 4 (over x, core), gz: 4 (over z).
Axes of the slice: x: 2, y: 2, z: 4, core: 2. Of those that a mesh axis runs over, the one named last changes fastest.
Arguments:
- rhs_velocity: float32 [3, 8, 32, 512], P(None, 'gx', 'gy', 'gz'), may hold values from -6 to 6
- rhs_pressure: float32 [8, 32, 512], P('gx', 'gy', 'gz'), may hold values from -6 to 6
- layer_ids: int32 [8, 32, 512], P('gx', 'gy', 'gz'), may hold values from 0 to 7
- visc_table: float32 [8], replicated, may hold values from 0.5 to 8
- stencil: float32 [27, 3, 3], replicated, as said below
Outputs:
- velocity_out: float32 [3, 8, 32, 512], P(None, 'gx', 'gy', 'gz')
- pressure_out: float32 [8, 32, 512], P('gx', 'gy', 'gz')
The draws below stay inside these ranges and needn't reach their ends.
Inputs may be any that keep to these rules, and one draw needn't show every extreme that they name: The block stencil[13] has a positive diagonal that dominates its row together with all other blocks' entries.
All inputs are finite; a program needn't handle non-finite values.
Results may differ from the reference program's by a relative error of at most 0.00015.
Values sent between devices are 32-bit elements; how exact they have to be, the bound alone decides.
A program may use at most 64 MiB of HBM per device.

```python
import math
import jax
import jax.numpy as jnp
from jax import lax

LAYERS = 8
NX = 8
NY = 32
NZ = 512


def draw_stencil(key, part):
    key_off = jax.random.fold_in(key, 11)
    key_mid = jax.random.fold_in(key, 12)
    key_diag = jax.random.fold_in(key, 13)
    spread = 0.03
    others = jax.random.normal(key_off, (27, 3, 3), jnp.float32) * spread
    center_off = jax.random.normal(key_mid, (3, 3), jnp.float32) * 0.1
    picker = (jnp.arange(27) == 13).astype(jnp.float32)[:, None, None]
    others = others * (1.0 - picker)
    eye = jnp.eye(3, dtype=jnp.float32)
    row_mass = jnp.sum(jnp.abs(others), axis=(0, 2)) + jnp.sum(jnp.abs(center_off * (1.0 - eye)), axis=1)
    extra = jax.random.uniform(key_diag, (3,), jnp.float32, 0.0, 0.5)
    center = center_off * (1.0 - eye) + eye * (1.0 + row_mass + extra)[:, None]
    return others + picker * center[None]


def place_ends(drawn, rng, low, largest):
    shape = drawn.shape
    index_at = [jax.random.randint(jax.random.fold_in(rng, axis), (), 0, shape[axis]) for axis in range(len(shape))]
    drawn = drawn.at[tuple(index_at)].set(low)
    longest = shape.index(max(shape))
    index_at[longest] = (index_at[longest] + 1) % shape[longest]
    return drawn.at[tuple(index_at)].set(largest)


def block_scale(rng, extent, shards, low, largest):
    gain = 1.0
    for dim, shards_of in shards:
        heights = jax.random.uniform(jax.random.fold_in(jax.random.fold_in(rng, 6), dim), (shards_of,), jnp.float32, low / len(shards), largest / len(shards))
        gain = gain * jnp.repeat(jnp.exp(heights), extent[dim] // shards_of).reshape((-1,) + (1,) * (len(extent) - 1 - dim))
    return gain


def normal_values(key, dims, scale, bound, shards=(), held_as=jnp.bfloat16):
    factor_of = block_scale(key, dims, shards, -0.22, 0.18) if shards else 1.0
    values = jax.random.normal(key, dims, jnp.float32) * scale * factor_of
    return jnp.minimum(jnp.maximum(values, -bound), bound).astype(held_as)


def setup_inputs(seed: int = 0) -> dict:
    arg_keys = jax.random.split(jax.random.key(seed), 6)
    return {
        "rhs_velocity": normal_values(arg_keys[0], (3, NX, NY, NZ), 1.0, 6.0, ((1, 2), (2, 4), (3, 4)), jnp.float32),
        "rhs_pressure": normal_values(arg_keys[1], (NX, NY, NZ), 1.0, 6.0, ((0, 2), (1, 4), (2, 4)), jnp.float32),
        "layer_ids": place_ends(jax.random.randint(arg_keys[2], (NX, NY, NZ), 0, LAYERS), jax.random.fold_in(arg_keys[2], 1), 0, LAYERS - 1).astype(jnp.int32),
        "visc_table": jnp.clip(jnp.exp(jax.random.uniform(arg_keys[3], (LAYERS,), jnp.float32, math.log(0.5), math.log(8.0))), 0.5, 8.0),
        "stencil": draw_stencil(jax.random.fold_in(arg_keys[5], 71), 0),
    }


LOW_BOUND = 0.2
HIGH_BOUND = 1.8
OMEGA = 2.0 / 3.0


def cheb_consts():
    theta = (HIGH_BOUND + LOW_BOUND) / 2.0
    delta = (HIGH_BOUND - LOW_BOUND) / 2.0
    sigma = theta / delta
    rho_zero = 1.0 / sigma
    rho_one = 1.0 / (2.0 * sigma - rho_zero)
    return theta, delta, rho_zero, rho_one


def stencil_sum(padded, stencil):
    sizes = (padded.shape[1] - 2, padded.shape[2] - 2, padded.shape[3] - 2)
    total = jnp.zeros((3,) + sizes, jnp.float32)
    for first in range(3):
        for second in range(3):
            for third in range(3):
                slab = padded[:, first:first + sizes[0], second:second + sizes[1], third:third + sizes[2]]
                block = stencil[first * 9 + second * 3 + third]
                total = total + jnp.einsum("ij,jxyz->ixyz", block, slab, precision=lax.Precision.HIGHEST)
    return total


def lookup(layer_ids, visc_table):
    eta = jnp.zeros(layer_ids.shape, jnp.float32)
    for layer in range(visc_table.shape[0]):
        eta = eta + jnp.where(layer_ids == layer, visc_table[layer], 0.0)
    return eta


def apply_field(field, scale, stencil):
    padded = jnp.pad(field, ((0, 0), (1, 1), (1, 1), (1, 1)))
    return scale[None] * stencil_sum(padded, stencil)


def smooth_zero(rhs, scale, dinv, stencil):
    theta, delta, rho_zero, rho_one = cheb_consts()
    first = dinv[None] * rhs / theta
    resid = rhs - apply_field(first, scale, stencil)
    second = rho_one * rho_zero * first + (2.0 * rho_one / delta) * dinv[None] * resid
    return first + second


def coarsen(field):
    shape = field.shape
    blocks = field.reshape(shape[:-3] + (shape[-3] // 2, 2, shape[-2] // 2, 2, shape[-1] // 2, 2))
    count = len(shape)
    return jnp.mean(blocks, axis=(count - 2, count, count + 2))


def refine(field):
    return jnp.repeat(jnp.repeat(jnp.repeat(field, 2, axis=1), 2, axis=2), 2, axis=3)


def reference(rhs_velocity, rhs_pressure, layer_ids, visc_table, stencil):
    theta, delta, rho_zero, rho_one = cheb_consts()
    eta = lookup(layer_ids, visc_table)
    kc = (stencil[13, 0, 0] + stencil[13, 1, 1] + stencil[13, 2, 2]) / 3.0
    dinv = 1.0 / (eta * kc)
    smoothed = smooth_zero(rhs_velocity, eta, dinv, stencil)
    residual = rhs_velocity - apply_field(smoothed, eta, stencil)
    coarse_res = coarsen(residual)
    eta_coarse = coarsen(eta)
    scale_coarse = 0.25 * eta_coarse
    dinv_coarse = 1.0 / (scale_coarse * kc)
    correction = smooth_zero(coarse_res, scale_coarse, dinv_coarse, stencil)
    start = smoothed + refine(correction)
    resid = rhs_velocity - apply_field(start, eta, stencil)
    first = dinv[None] * resid / theta
    middle = start + first
    resid = rhs_velocity - apply_field(middle, eta, stencil)
    second = rho_one * rho_zero * first + (2.0 * rho_one / delta) * dinv[None] * resid
    velocity_out = middle + second
    weight = 1.0 / eta
    pinv = 1.0 / (6.0 * weight)
    pressure = OMEGA * pinv * rhs_pressure
    for sweep in range(2):
        padded = jnp.pad(pressure, 1)
        beside = padded[2:, 1:-1, 1:-1] + padded[:-2, 1:-1, 1:-1]
        beside = beside + padded[1:-1, 2:, 1:-1] + padded[1:-1, :-2, 1:-1]
        beside = beside + padded[1:-1, 1:-1, 2:] + padded[1:-1, 1:-1, :-2]
        applied = weight * (6.0 * pressure - beside)
        pressure = pressure + OMEGA * pinv * (rhs_pressure - applied)
    return velocity_out, pressure
```

```python
import functools
import jax
import jax.numpy as jnp
from jax import lax
from jax.experimental import pallas as pl
from jax.experimental.pallas import tpu as pltpu
from jax.sharding import PartitionSpec as P

LOW_BOUND = 0.2
HIGH_BOUND = 1.8
OMEGA = 2.0 / 3.0
THETA = (HIGH_BOUND + LOW_BOUND) / 2.0
DELTA = (HIGH_BOUND - LOW_BOUND) / 2.0
SIGMA = THETA / DELTA
RHO_ZERO = 1.0 / SIGMA
RHO_ONE = 1.0 / (2.0 * SIGMA - RHO_ZERO)
WEIGHT = 2.0 * RHO_ONE / DELTA
KEEP = RHO_ONE * RHO_ZERO
GAIN = 1.0 + KEEP + WEIGHT * THETA

DEPTH = 3
COARSE_DEPTH = 2
EDGE = 4
OFFSETS = [
    (dx, dy, dz)
    for dx in (-1, 0, 1)
    for dy in (-1, 0, 1)
    for dz in (-1, 0, 1)
    if (dx, dy, dz) != (0, 0, 0)
]


def roll(x, shift, axis):
    return pltpu.roll(x, shift % x.shape[axis], axis)


def side(d):
    return 0 if d < 0 else 1


class Halo:
    def __init__(self, planes, comps, depth, refs):
        self.n, self.c, self.d = planes, comps, depth
        self.own, self.yp, self.zp, self.xb, self.yb, self.xyb, self.zb, self.ss, self.rs = refs

    @staticmethod
    def shapes(planes, comps, depth, rows, lanes):
        half = planes * comps // 2
        slots = -(-planes * comps * 2 * EDGE // lanes)
        f32 = jnp.float32
        return [
            pltpu.VMEM((planes, comps, rows, lanes), f32),
            pltpu.VMEM((2, half, rows, lanes), f32),
            pltpu.VMEM((slots, rows, lanes), f32),
            pltpu.VMEM((2, depth, comps, rows, lanes), f32),
            pltpu.VMEM((2, half, rows, lanes), f32),
            pltpu.VMEM((2, 2, depth * comps // 2, rows, lanes), f32),
            pltpu.VMEM((3, 3, 2, slots, rows, lanes), f32),
            pltpu.SemaphoreType.DMA((len(OFFSETS),)),
            pltpu.SemaphoreType.DMA((len(OFFSETS),)),
        ]

    def clear(self):
        for ref in (self.xb, self.yb, self.xyb, self.zb):
            ref[...] = jnp.zeros(ref.shape, ref.dtype)

    def pack(self):
        rows, lanes = self.own.shape[2:]
        row = lax.broadcasted_iota(jnp.int32, (rows, lanes), 0)
        slot = lax.broadcasted_iota(jnp.int32, (rows, lanes), 1) // (2 * EDGE)
        flat = [self.own[k, c] for k in range(self.n) for c in range(self.c)]
        for q in range(len(flat) // 2):
            even, odd = flat[2 * q], roll(flat[2 * q + 1], EDGE, 0)
            self.yp[0, q] = jnp.where(row < EDGE, even, odd)
            self.yp[1, q] = jnp.where(row < EDGE, odd, even)
        per = lanes // (2 * EDGE)
        for first in range(0, len(flat), per):
            strip = jnp.zeros((rows, lanes), jnp.float32)
            for s, v in enumerate(flat[first : first + per]):
                strip = jnp.where(slot == s, roll(v, s * 2 * EDGE + EDGE, 1), strip)
            self.zp[first // per] = strip

    def copy(self, index, me, receive):
        dx, dy, dz = OFFSETS[index]
        lo = 0 if dx < 0 else self.n - self.d
        half = self.d * self.c // 2
        rx, ry, rz = (dx, dy, dz) if receive else (-dx, -dy, -dz)
        if dz:
            src, dst = self.zp, self.zb.at[rx + 1, ry + 1, side(rz)]
        elif dx and dy:
            src = self.yp.at[side(dy), pl.ds(lo * self.c // 2, half)]
            dst = self.xyb.at[side(rx), side(ry)]
        elif dx:
            src, dst = self.own.at[pl.ds(lo, self.d)], self.xb.at[side(rx)]
        else:
            src, dst = self.yp.at[side(dy)], self.yb.at[side(ry)]
        arrival = index if receive else len(OFFSETS) - 1 - index
        return pltpu.make_async_remote_copy(
            src_ref=src,
            dst_ref=dst,
            send_sem=self.ss.at[index],
            recv_sem=self.rs.at[arrival],
            device_id=target(me, OFFSETS[index]),
            device_id_type=pl.DeviceIdType.MESH,
        )

    def send(self, me, exists):
        for index in ORDER:
            @pl.when(exists[index])
            def _():
                self.copy(index, me, False).start()

    def arrive(self, me, exists):
        for index in ORDER:
            @pl.when(exists[index])
            def _():
                self.copy(index, me, True).wait_recv()

    def drain(self, me, exists):
        for index in ORDER:
            @pl.when(exists[index])
            def _():
                self.copy(index, me, False).wait_send()

    def unpack(self, out):
        rows, lanes = self.own.shape[2:]
        row = lax.broadcasted_iota(jnp.int32, (rows, lanes), 0)
        lane = lax.broadcasted_iota(jnp.int32, (rows, lanes), 1)
        high = lane % (2 * EDGE) < EDGE
        per = lanes // (2 * EDGE)
        half = self.d * self.c // 2
        skip = (self.n - self.d) * self.c // 2
        for dx in (-1, 0, 1):
            strips = []
            for t in range(self.zp.shape[0]):
                at = [
                    jnp.where(high, self.zb[dx + 1, dy + 1, 0, t], self.zb[dx + 1, dy + 1, 1, t])
                    for dy in (-1, 0, 1)
                ]
                strips.append((at[1], jnp.where(row < EDGE, at[2], at[0])))
            first = self.n - self.d if dx < 0 else 0
            last = self.d if dx > 0 else self.n
            for k in range(first, last):
                p = k + self.d + dx * self.n
                for c in range(self.c):
                    idx = k * self.c + c
                    q = idx // 2
                    if dx == 0:
                        main, minus, plus = self.own[k, c], self.yb[0, q], self.yb[1, q]
                    else:
                        s = side(dx)
                        b = skip if dx < 0 else 0
                        main = self.xb[s, k - first, c]
                        minus, plus = self.xyb[s, 0, q - b], self.xyb[s, 1, q - b]
                    if idx % 2 == 0:
                        beside = jnp.where(row < EDGE, plus, minus)
                    else:
                        beside = roll(jnp.where(row < EDGE, minus, plus), EDGE, 0)
                    back = -((idx % per) * 2 * EDGE + EDGE)
                    mid, far = strips[idx // per]
                    out[p, c, :rows, :lanes] = main
                    out[p, c, :rows, lanes:] = roll(mid, back, 1)
                    out[p, c, rows:, :lanes] = beside
                    out[p, c, rows:, lanes:] = roll(far, back, 1)


ORDER = sorted(range(len(OFFSETS)), key=lambda i: -sum(abs(d) for d in OFFSETS[i]))


def target(me, offset):
    return {axis: at + d for (axis, at), d in zip(me.items(), offset)}


def stencil_wide(ref, p, st, step):
    rows = ref.shape[2]
    lanes = ref.shape[3]
    total = [[None] * 3 for _ in range(3)]
    for a in range(3):
        for j in range(3):
            v = ref[p + a - 1, j]
            for c, w in enumerate((roll(v, step, 1), v, roll(v, lanes - step, 1))):
                for i in range(3):
                    for b in range(3):
                        term = st[(a * 9 + b * 3 + c) * 9 + i * 3 + j] * w
                        total[i][b] = term if total[i][b] is None else total[i][b] + term
    return [
        total[i][1] + roll(total[i][0], step, 0) + roll(total[i][2], rows - step, 0)
        for i in range(3)
    ]


def stencil_own(ref, p, st):
    rows, lanes = ref.shape[2], ref.shape[3]
    total = [None] * 3
    for a in range(3):
        for j in range(3):
            v = ref[p + a - 1, j]
            for c in range(3):
                w = roll(v, (1 - c) % lanes, 1) if c != 1 else v
                w = w[:, : lanes // 2]
                for b in range(3):
                    u = (roll(w, (1 - b) % rows, 0) if b != 1 else w)[: rows // 2]
                    for i in range(3):
                        term = st[(a * 9 + b * 3 + c) * 9 + i * 3 + j] * u
                        total[i] = term if total[i] is None else total[i] + term
    return total


def kernel(sizes, rv, rp, ids, table, st, vout, pout, *scratch):
    planes, rows, lanes = ids.shape
    fine = Halo(planes, 4, DEPTH, scratch[:9])
    coarse = Halo(planes // 2, 3, COARSE_DEPTH, scratch[9:18])
    wide, smooth, cwide, middle, press, eta_ref = scratch[18:]
    me = {axis: lax.axis_index(axis) for axis in sizes}
    exists = []
    for offset in OFFSETS:
        ok = None
        for (axis, at), d in zip(me.items(), offset):
            if d:
                one = at > 0 if d < 0 else at < sizes[axis] - 1
                ok = one if ok is None else jnp.logical_and(ok, one)
        exists.append(ok)

    fine.clear()
    coarse.clear()
    barrier = pltpu.get_barrier_semaphore()
    for index in ORDER:
        @pl.when(exists[index])
        def _():
            pl.semaphore_signal(
                barrier,
                inc=1,
                device_id=target(me, OFFSETS[index]),
                device_id_type=pl.DeviceIdType.MESH,
            )

    kc = jnp.full((rows, lanes), (st[117] + st[121] + st[125]) / 3.0, jnp.float32)
    inv_kc = 1.0 / kc
    inv_wide = jnp.tile(inv_kc, (2, 2))
    for k in range(planes):
        eta = jnp.zeros((rows, lanes), jnp.float32)
        for layer in range(table.shape[0]):
            eta = jnp.where(ids[k] == layer, table[layer], eta)
        eta_ref[k] = eta
        dinv = 1.0 / (eta * kc)
        for i in range(3):
            fine.own[k, i] = dinv * rv[i, k] / THETA
        fine.own[k, 3] = (OMEGA / 6.0) * eta * rp[k]
    fine.pack()
    peers = 1
    for axis, at in me.items():
        peers = peers * (
            1 + (at > 0).astype(jnp.int32) + (at < sizes[axis] - 1).astype(jnp.int32)
        )
    pl.semaphore_wait(barrier, peers - 1)
    fine.send(me, exists)

    row = lax.broadcasted_iota(jnp.int32, (2 * rows, 2 * lanes), 0)
    lane = lax.broadcasted_iota(jnp.int32, (2 * rows, 2 * lanes), 1)
    gx, gy, gz = sizes
    has_low = {axis: (me[axis] > 0).astype(jnp.float32) for axis in sizes}
    has_high = {axis: (me[axis] < sizes[axis] - 1).astype(jnp.float32) for axis in sizes}
    mask = jnp.where(row < rows, 1.0, jnp.where(row < rows + EDGE, has_high[gy], has_low[gy]))
    mask = mask * jnp.where(
        lane < lanes, 1.0, jnp.where(lane < lanes + lanes // 2, has_high[gz], has_low[gz])
    )

    def plane_mask(x):
        inside = jnp.where(x < 0, has_low[gx], jnp.where(x >= planes, has_high[gx], 1.0))
        return mask * inside

    fine.arrive(me, exists)
    fine.unpack(wide)

    def smoothing(x):
        m = plane_mask(x)
        sums = stencil_wide(wide, x + DEPTH, st, 1)
        for i in range(3):
            smooth[x + 2, i] = (GAIN * wide[x + DEPTH, i] - (WEIGHT * inv_wide) * sums[i]) * m

    @pl.loop(-1, planes + 1)
    def _(x):
        smoothing(x)

    even_row = lax.broadcasted_iota(jnp.int32, (rows, lanes), 0) % 2 == 0
    even_lane = lax.broadcasted_iota(jnp.int32, (rows, lanes), 1) % 2 == 0

    def pair_sum(v):
        v = v + jnp.where(even_row, roll(v, rows - 1, 0), roll(v, 1, 0))
        return v + jnp.where(even_lane, roll(v, lanes - 1, 1), roll(v, 1, 1))

    @pl.loop(0, planes // 2)
    def _(h):
        parts = [None] * 3
        eta_sum = None
        for half in range(2):
            x = 2 * h + half
            eta = eta_ref[x]
            eta_sum = eta if eta_sum is None else eta_sum + eta
            sums = stencil_own(smooth, x + 2, st)
            for i in range(3):
                value = eta * ((kc * THETA) * fine.own[x, i] - sums[i])
                parts[i] = value if parts[i] is None else parts[i] + value
        dinv_c = 4.0 / (pair_sum(eta_sum) * kc * THETA)
        for i in range(3):
            coarse.own[h, i] = dinv_c * pair_sum(parts[i])

    coarse.pack()
    coarse.send(me, exists)

    smoothing(-2)
    smoothing(planes + 1)

    def star(ref, x):
        v = ref(x)
        total = ref(x - 1) + ref(x + 1)
        total = total + roll(v, 1, 0) + roll(v, 2 * rows - 1, 0)
        return total + roll(v, 1, 1) + roll(v, 2 * lanes - 1, 1)

    @pl.loop(-1, planes + 1)
    def _(x):
        near = star(lambda k: wide[k + DEPTH, 3], x)
        press[x + 1] = ((2.0 - OMEGA) * wide[x + DEPTH, 3] + (OMEGA / 6.0) * near) * plane_mask(x)

    @pl.loop(0, planes)
    def _(x):
        near = star(lambda k: press[k + 1], x)
        value = wide[x + DEPTH, 3] + (1.0 - OMEGA) * press[x + 1] + (OMEGA / 6.0) * near
        pout[x] = value[:rows, :lanes]

    coarse.arrive(me, exists)
    coarse.unpack(cwide)

    @pl.loop(-1, planes // 2 + 1)
    def _(h):
        sums = stencil_wide(cwide, h + COARSE_DEPTH, st, 2)
        m = plane_mask(2 * h)
        for i in range(3):
            value = GAIN * cwide[h + COARSE_DEPTH, i] - (WEIGHT * inv_wide) * sums[i]
            value = value * m
            smooth[2 * h + 2, i] += value
            smooth[2 * h + 3, i] += value

    @pl.loop(-1, planes + 1)
    def _(x):
        m = plane_mask(x)
        sums = stencil_wide(smooth, x + 2, st, 1)
        for i in range(3):
            first = wide[x + DEPTH, i] - (inv_wide / THETA) * sums[i]
            middle[x + 1, i] = smooth[x + 2, i] + first * m

    @pl.loop(0, planes)
    def _(x):
        sums = stencil_own(middle, x + 1, st)
        for i in range(3):
            mid = middle[x + 1, i, :rows, :lanes]
            first = mid - smooth[x + 2, i, :rows, :lanes]
            scaled = (WEIGHT * THETA) * fine.own[x, i] - (WEIGHT * inv_kc) * sums[i]
            vout[i, x] = mid + KEEP * first + scaled

    fine.drain(me, exists)
    coarse.drain(me, exists)


def on_device(sizes, rhs_velocity, rhs_pressure, layer_ids, visc_table, stencil):
    planes, rows, lanes = layer_ids.shape
    f32 = jnp.float32
    vmem = pl.BlockSpec(memory_space=pltpu.VMEM)
    smem = pl.BlockSpec(memory_space=pltpu.SMEM)
    return pl.pallas_call(
        functools.partial(kernel, sizes),
        out_shape=(
            jax.ShapeDtypeStruct(rhs_velocity.shape, f32),
            jax.ShapeDtypeStruct(rhs_pressure.shape, f32),
        ),
        in_specs=[vmem, vmem, vmem, smem, smem],
        out_specs=(vmem, vmem),
        scratch_shapes=[
            *Halo.shapes(planes, 4, DEPTH, rows, lanes),
            *Halo.shapes(planes // 2, 3, COARSE_DEPTH, rows, lanes),
            pltpu.VMEM((planes + 2 * DEPTH, 4, 2 * rows, 2 * lanes), f32),
            pltpu.VMEM((planes + 4, 3, 2 * rows, 2 * lanes), f32),
            pltpu.VMEM((planes // 2 + 2 * COARSE_DEPTH, 3, 2 * rows, 2 * lanes), f32),
            pltpu.VMEM((planes + 2, 3, 2 * rows, 2 * lanes), f32),
            pltpu.VMEM((planes + 2, 2 * rows, 2 * lanes), f32),
            pltpu.VMEM((planes, rows, lanes), f32),
        ],
        compiler_params=pltpu.CompilerParams(collective_id=0, has_side_effects=True),
        name="stokes",
    )(rhs_velocity, rhs_pressure, layer_ids, visc_table, stencil.reshape(-1))


def solution(mesh):
    placed = (P(None, "gx", "gy", "gz"), P("gx", "gy", "gz"), P("gx", "gy", "gz"), P(), P())
    sizes = {axis: mesh.shape[axis] for axis in ("gx", "gy", "gz")}
    return jax.shard_map(
        functools.partial(on_device, sizes),
        mesh=mesh,
        in_specs=placed,
        out_specs=(P(None, "gx", "gy", "gz"), P("gx", "gy", "gz")),
        check_vma=False,
    )
```

```python
import functools
import jax
import jax.numpy as jnp
from jax import lax
from jax.experimental import pallas as pl
from jax.experimental.pallas import tpu as pltpu
from jax.sharding import PartitionSpec as P

LOW_BOUND = 0.2
HIGH_BOUND = 1.8
OMEGA = 2.0 / 3.0
THETA = (HIGH_BOUND + LOW_BOUND) / 2.0
DELTA = (HIGH_BOUND - LOW_BOUND) / 2.0
SIGMA = THETA / DELTA
RHO_ZERO = 1.0 / SIGMA
RHO_ONE = 1.0 / (2.0 * SIGMA - RHO_ZERO)
WEIGHT = 2.0 * RHO_ONE / DELTA
KEEP = RHO_ONE * RHO_ZERO
GAIN = 1.0 + KEEP + WEIGHT * THETA

DEPTH = 3
COARSE_DEPTH = 2
EDGE = 4
OFFSETS = [
    (dx, dy, dz)
    for dx in (-1, 0, 1)
    for dy in (-1, 0, 1)
    for dz in (-1, 0, 1)
    if (dx, dy, dz) != (0, 0, 0)
]


def roll(x, shift, axis):
    return pltpu.roll(x, shift % x.shape[axis], axis)


def side(d):
    return 0 if d < 0 else 1


class Halo:
    def __init__(self, planes, comps, depth, refs):
        self.n, self.c, self.d = planes, comps, depth
        self.own, self.yp, self.zp, self.xb, self.yb, self.xyb, self.zb, self.ss, self.rs = refs

    @staticmethod
    def shapes(planes, comps, depth, rows, lanes):
        half = planes * comps // 2
        slots = -(-planes * comps * 2 * EDGE // lanes)
        f32 = jnp.float32
        return [
            pltpu.VMEM((planes, comps, rows, lanes), f32),
            pltpu.VMEM((2, half, rows, lanes), f32),
            pltpu.VMEM((slots, rows, lanes), f32),
            pltpu.VMEM((2, depth, comps, rows, lanes), f32),
            pltpu.VMEM((2, half, rows, lanes), f32),
            pltpu.VMEM((2, 2, depth * comps // 2, rows, lanes), f32),
            pltpu.VMEM((3, 3, 2, slots, rows, lanes), f32),
            pltpu.SemaphoreType.DMA((len(OFFSETS),)),
            pltpu.SemaphoreType.DMA((len(OFFSETS),)),
        ]

    def clear(self):
        for ref in (self.xb, self.yb, self.xyb, self.zb):
            ref[...] = jnp.zeros(ref.shape, ref.dtype)

    def pack(self):
        rows, lanes = self.own.shape[2:]
        row = lax.broadcasted_iota(jnp.int32, (rows, lanes), 0)
        slot = lax.broadcasted_iota(jnp.int32, (rows, lanes), 1) // (2 * EDGE)
        flat = [self.own[k, c] for k in range(self.n) for c in range(self.c)]
        for q in range(len(flat) // 2):
            even, odd = flat[2 * q], roll(flat[2 * q + 1], EDGE, 0)
            self.yp[0, q] = jnp.where(row < EDGE, even, odd)
            self.yp[1, q] = jnp.where(row < EDGE, odd, even)
        per = lanes // (2 * EDGE)
        for first in range(0, len(flat), per):
            strip = jnp.zeros((rows, lanes), jnp.float32)
            for s, v in enumerate(flat[first : first + per]):
                strip = jnp.where(slot == s, roll(v, s * 2 * EDGE + EDGE, 1), strip)
            self.zp[first // per] = strip

    def copy(self, index, me, receive):
        dx, dy, dz = OFFSETS[index]
        lo = 0 if dx < 0 else self.n - self.d
        half = self.d * self.c // 2
        rx, ry, rz = (dx, dy, dz) if receive else (-dx, -dy, -dz)
        if dz:
            src, dst = self.zp, self.zb.at[rx + 1, ry + 1, side(rz)]
        elif dx and dy:
            src = self.yp.at[side(dy), pl.ds(lo * self.c // 2, half)]
            dst = self.xyb.at[side(rx), side(ry)]
        elif dx:
            src, dst = self.own.at[pl.ds(lo, self.d)], self.xb.at[side(rx)]
        else:
            src, dst = self.yp.at[side(dy)], self.yb.at[side(ry)]
        arrival = index if receive else len(OFFSETS) - 1 - index
        return pltpu.make_async_remote_copy(
            src_ref=src,
            dst_ref=dst,
            send_sem=self.ss.at[index],
            recv_sem=self.rs.at[arrival],
            device_id=target(me, OFFSETS[index]),
            device_id_type=pl.DeviceIdType.MESH,
        )

    def send(self, me, exists):
        for index in ORDER:
            @pl.when(exists[index])
            def _():
                self.copy(index, me, False).start()

    def arrive(self, me, exists):
        for index in ORDER:
            @pl.when(exists[index])
            def _():
                self.copy(index, me, True).wait_recv()

    def drain(self, me, exists):
        for index in ORDER:
            @pl.when(exists[index])
            def _():
                self.copy(index, me, False).wait_send()

    def unpack(self, out):
        rows, lanes = self.own.shape[2:]
        row = lax.broadcasted_iota(jnp.int32, (rows, lanes), 0)
        lane = lax.broadcasted_iota(jnp.int32, (rows, lanes), 1)
        high = lane % (2 * EDGE) < EDGE
        per = lanes // (2 * EDGE)
        half = self.d * self.c // 2
        skip = (self.n - self.d) * self.c // 2
        for dx in (-1, 0, 1):
            strips = []
            for t in range(self.zp.shape[0]):
                at = [
                    jnp.where(high, self.zb[dx + 1, dy + 1, 0, t], self.zb[dx + 1, dy + 1, 1, t])
                    for dy in (-1, 0, 1)
                ]
                strips.append((at[1], jnp.where(row < EDGE, at[2], at[0])))
            first = self.n - self.d if dx < 0 else 0
            last = self.d if dx > 0 else self.n
            for k in range(first, last):
                p = k + self.d + dx * self.n
                for c in range(self.c):
                    idx = k * self.c + c
                    q = idx // 2
                    if dx == 0:
                        main, minus, plus = self.own[k, c], self.yb[0, q], self.yb[1, q]
                    else:
                        s = side(dx)
                        b = skip if dx < 0 else 0
                        main = self.xb[s, k - first, c]
                        minus, plus = self.xyb[s, 0, q - b], self.xyb[s, 1, q - b]
                    if idx % 2 == 0:
                        beside = jnp.where(row < EDGE, plus, minus)
                    else:
                        beside = roll(jnp.where(row < EDGE, minus, plus), EDGE, 0)
                    back = -((idx % per) * 2 * EDGE + EDGE)
                    mid, far = strips[idx // per]
                    out[p, c, :rows, :lanes] = main
                    out[p, c, :rows, lanes:] = roll(mid, back, 1)
                    out[p, c, rows:, :lanes] = beside
                    out[p, c, rows:, lanes:] = roll(far, back, 1)


ORDER = sorted(range(len(OFFSETS)), key=lambda i: -sum(abs(d) for d in OFFSETS[i]))


def target(me, offset):
    return {axis: at + d for (axis, at), d in zip(me.items(), offset)}


def coupling(st, rows, step):
    parts = 3 * rows
    width = 9 * parts
    padded = -(-width // 128) * 128
    row = lax.broadcasted_iota(jnp.int32, (rows, padded), 0)
    lane = lax.broadcasted_iota(jnp.int32, (rows, padded), 1)
    head = lax.broadcasted_iota(jnp.int32, (8, padded), 1)
    pair = (head // (3 * parts)) * 3 + (head % parts) // rows
    low = (lane % (3 * parts)) // parts == 2
    moved = (lane % rows - row + rows) % rows
    bands = [moved == (step * (b - 1)) % rows for b in range(3)]
    blocks = []
    for c in range(3):
        for i in range(3):
            block = jnp.zeros((rows, padded), jnp.float32)
            for b in range(3):
                line = jnp.zeros((8, padded), jnp.float32)
                for a in range(3):
                    for j in range(3):
                        line = jnp.where(pair == a * 3 + j, st[i, j, a * 9 + b * 3 + c], line)
                block = jnp.where(bands[b], jnp.tile(line, (rows // 8, 1)), block)
            high = block.astype(jnp.bfloat16).astype(jnp.float32)
            blocks.append(jnp.where(low, block - high, high))
    return blocks


def put(parts, p, j, v):
    rows = v.shape[0]
    high = v.astype(jnp.bfloat16)
    low = (v - high.astype(jnp.float32)).astype(jnp.bfloat16)
    parts[p, 0, j] = high
    parts[p, 1, j] = low
    parts[p, 2, j] = high


def product(matrix, parts, p):
    depth = 3 * 9 * parts.shape[3]
    window = parts[pl.ds(p - 1, 3)].reshape(depth, parts.shape[4])
    return jnp.dot(matrix[:, :depth], window, preferred_element_type=jnp.float32)


def stencil(matrix, parts, p, rows, step):
    lanes = parts.shape[4]
    r = product(matrix, parts, p)
    at = lambda c, i: r[(c * 3 + i) * rows : (c * 3 + i + 1) * rows]
    return [at(1, i) + roll(at(0, i), step, 1) + roll(at(2, i), lanes - step, 1) for i in range(3)]


def kernel(sizes, rv, rp, ids, table, st, vout, pout, *scratch):
    planes, rows, lanes = ids.shape
    fine = Halo(planes, 4, DEPTH, scratch[:9])
    coarse = Halo(planes // 2, 3, COARSE_DEPTH, scratch[9:18])
    wide, smooth, cwide, middle, press, eta_ref = scratch[18:24]
    wide_p, smooth_p, cwide_p, middle_p, m_wide, m_own, m_coarse = scratch[24:]
    tall = 2 * rows
    me = {axis: lax.axis_index(axis) for axis in sizes}
    exists = []
    for offset in OFFSETS:
        ok = None
        for (axis, at), d in zip(me.items(), offset):
            if d:
                one = at > 0 if d < 0 else at < sizes[axis] - 1
                ok = one if ok is None else jnp.logical_and(ok, one)
        exists.append(ok)

    fine.clear()
    coarse.clear()
    barrier = pltpu.get_barrier_semaphore()
    for index in ORDER:
        @pl.when(exists[index])
        def _():
            pl.semaphore_signal(
                barrier,
                inc=1,
                device_id=target(me, OFFSETS[index]),
                device_id_type=pl.DeviceIdType.MESH,
            )

    kc = jnp.full((rows, lanes), (st[0, 0, 13] + st[1, 1, 13] + st[2, 2, 13]) / 3.0, jnp.float32)
    inv_kc = 1.0 / kc
    inv_wide = jnp.tile(inv_kc, (2, 2))
    for k in range(planes):
        eta = jnp.zeros((rows, lanes), jnp.float32)
        for layer in range(table.shape[0]):
            eta = jnp.where(ids[k] == layer, table[layer], eta)
        eta_ref[k] = eta
        dinv = 1.0 / (eta * kc)
        for i in range(3):
            fine.own[k, i] = dinv * rv[i, k] / THETA
        fine.own[k, 3] = (OMEGA / 6.0) * eta * rp[k]
    fine.pack()
    peers = 1
    for axis, at in me.items():
        peers = peers * (
            1 + (at > 0).astype(jnp.int32) + (at < sizes[axis] - 1).astype(jnp.int32)
        )
    pl.semaphore_wait(barrier, peers - 1)
    fine.send(me, exists)

    blocks = coupling(st, tall, 1)
    m_wide[...] = jnp.concatenate(blocks, axis=0).astype(jnp.bfloat16)
    m_own[...] = jnp.concatenate([b[:rows] for b in blocks], axis=0).astype(jnp.bfloat16)

    row = lax.broadcasted_iota(jnp.int32, (2 * rows, 2 * lanes), 0)
    lane = lax.broadcasted_iota(jnp.int32, (2 * rows, 2 * lanes), 1)
    gx, gy, gz = sizes
    has_low = {axis: (me[axis] > 0).astype(jnp.float32) for axis in sizes}
    has_high = {axis: (me[axis] < sizes[axis] - 1).astype(jnp.float32) for axis in sizes}
    mask = jnp.where(row < rows, 1.0, jnp.where(row < rows + EDGE, has_high[gy], has_low[gy]))
    mask = mask * jnp.where(
        lane < lanes, 1.0, jnp.where(lane < lanes + lanes // 2, has_high[gz], has_low[gz])
    )

    def plane_mask(x):
        inside = jnp.where(x < 0, has_low[gx], jnp.where(x >= planes, has_high[gx], 1.0))
        return mask * inside

    fine.arrive(me, exists)
    fine.unpack(wide)
    for p in range(planes + 2 * DEPTH):
        for j in range(3):
            put(wide_p, p, j, wide[p, j])

    def smoothing(x):
        m = plane_mask(x)
        sums = stencil(m_wide, wide_p, x + DEPTH, tall, 1)
        for i in range(3):
            value = (GAIN * wide[x + DEPTH, i] - (WEIGHT * inv_wide) * sums[i]) * m
            smooth[x + 2, i] = value
            put(smooth_p, x + 2, i, value)

    @pl.loop(-1, planes + 1)
    def _(x):
        smoothing(x)

    even_row = lax.broadcasted_iota(jnp.int32, (rows, lanes), 0) % 2 == 0
    even_lane = lax.broadcasted_iota(jnp.int32, (rows, lanes), 1) % 2 == 0

    def pair_sum(v):
        v = v + jnp.where(even_row, roll(v, rows - 1, 0), roll(v, 1, 0))
        return v + jnp.where(even_lane, roll(v, lanes - 1, 1), roll(v, 1, 1))

    @pl.loop(0, planes // 2)
    def _(h):
        parts = [None] * 3
        eta_sum = None
        for half in range(2):
            x = 2 * h + half
            eta = eta_ref[x]
            eta_sum = eta if eta_sum is None else eta_sum + eta
            sums = stencil(m_own, smooth_p, x + 2, rows, 1)
            for i in range(3):
                value = eta * ((kc * THETA) * fine.own[x, i] - sums[i][:, :lanes])
                parts[i] = value if parts[i] is None else parts[i] + value
        dinv_c = 4.0 / (pair_sum(eta_sum) * kc * THETA)
        for i in range(3):
            coarse.own[h, i] = dinv_c * pair_sum(parts[i])

    coarse.pack()
    coarse.send(me, exists)

    m_coarse[...] = jnp.concatenate(coupling(st, tall, 2), axis=0).astype(jnp.bfloat16)
    smoothing(-2)
    smoothing(planes + 1)

    def star(ref, x):
        v = ref(x)
        total = ref(x - 1) + ref(x + 1)
        total = total + roll(v, 1, 0) + roll(v, 2 * rows - 1, 0)
        return total + roll(v, 1, 1) + roll(v, 2 * lanes - 1, 1)

    @pl.loop(-1, planes + 1)
    def _(x):
        near = star(lambda k: wide[k + DEPTH, 3], x)
        press[x + 1] = ((2.0 - OMEGA) * wide[x + DEPTH, 3] + (OMEGA / 6.0) * near) * plane_mask(x)

    @pl.loop(0, planes)
    def _(x):
        near = star(lambda k: press[k + 1], x)
        value = wide[x + DEPTH, 3] + (1.0 - OMEGA) * press[x + 1] + (OMEGA / 6.0) * near
        pout[x] = value[:rows, :lanes]

    coarse.arrive(me, exists)
    coarse.unpack(cwide)
    for p in range(planes // 2 + 2 * COARSE_DEPTH):
        for j in range(3):
            put(cwide_p, p, j, cwide[p, j])

    @pl.loop(-1, planes // 2 + 1)
    def _(h):
        sums = stencil(m_coarse, cwide_p, h + COARSE_DEPTH, tall, 2)
        m = plane_mask(2 * h)
        for i in range(3):
            value = GAIN * cwide[h + COARSE_DEPTH, i] - (WEIGHT * inv_wide) * sums[i]
            value = value * m
            for half in range(2):
                start = smooth[2 * h + 2 + half, i] + value
                smooth[2 * h + 2 + half, i] = start
                put(smooth_p, 2 * h + 2 + half, i, start)

    @pl.loop(-1, planes + 1)
    def _(x):
        m = plane_mask(x)
        sums = stencil(m_wide, smooth_p, x + 2, tall, 1)
        for i in range(3):
            first = wide[x + DEPTH, i] - (inv_wide / THETA) * sums[i]
            value = smooth[x + 2, i] + first * m
            middle[x + 1, i] = value[:rows, :lanes]
            put(middle_p, x + 1, i, value)

    @pl.loop(0, planes)
    def _(x):
        sums = stencil(m_own, middle_p, x + 1, rows, 1)
        for i in range(3):
            mid = middle[x + 1, i]
            first = mid - smooth[x + 2, i, :rows, :lanes]
            scaled = (WEIGHT * THETA) * fine.own[x, i] - (WEIGHT * inv_kc) * sums[i][:, :lanes]
            vout[i, x] = mid + KEEP * first + scaled

    fine.drain(me, exists)
    coarse.drain(me, exists)


def on_device(sizes, rhs_velocity, rhs_pressure, layer_ids, visc_table, stencil):
    planes, rows, lanes = layer_ids.shape
    f32 = jnp.float32
    columns = -(-54 * rows // 128) * 128
    vmem = pl.BlockSpec(memory_space=pltpu.VMEM)
    smem = pl.BlockSpec(memory_space=pltpu.SMEM)
    return pl.pallas_call(
        functools.partial(kernel, sizes),
        out_shape=(
            pltpu.VMEM(rhs_velocity.shape, f32),
            pltpu.VMEM(rhs_pressure.shape, f32),
        ),
        in_specs=[vmem, vmem, vmem, smem, smem],
        out_specs=(vmem, vmem),
        scratch_shapes=[
            *Halo.shapes(planes, 4, DEPTH, rows, lanes),
            *Halo.shapes(planes // 2, 3, COARSE_DEPTH, rows, lanes),
            pltpu.VMEM((planes + 2 * DEPTH, 4, 2 * rows, 2 * lanes), f32),
            pltpu.VMEM((planes + 4, 3, 2 * rows, 2 * lanes), f32),
            pltpu.VMEM((planes // 2 + 2 * COARSE_DEPTH, 3, 2 * rows, 2 * lanes), f32),
            pltpu.VMEM((planes + 2, 3, rows, lanes), f32),
            pltpu.VMEM((planes + 2, 2 * rows, 2 * lanes), f32),
            pltpu.VMEM((planes, rows, lanes), f32),
            *(
                pltpu.VMEM((count, 3, 3, 2 * rows, 2 * lanes), jnp.bfloat16)
                for count in (
                    planes + 2 * DEPTH,
                    planes + 4,
                    planes // 2 + 2 * COARSE_DEPTH,
                    planes + 2,
                )
            ),
            pltpu.VMEM((18 * rows, columns), jnp.bfloat16),
            pltpu.VMEM((9 * rows, columns), jnp.bfloat16),
            pltpu.VMEM((18 * rows, columns), jnp.bfloat16),
        ],
        compiler_params=pltpu.CompilerParams(collective_id=0, has_side_effects=True),
        name="stokes",
    )(rhs_velocity, rhs_pressure, layer_ids, visc_table, jnp.transpose(stencil, (1, 2, 0)))


def solution(mesh):
    placed = (P(None, "gx", "gy", "gz"), P("gx", "gy", "gz"), P("gx", "gy", "gz"), P(), P())
    sizes = {axis: mesh.shape[axis] for axis in ("gx", "gy", "gz")}
    return jax.shard_map(
        functools.partial(on_device, sizes),
        mesh=mesh,
        in_specs=placed,
        out_specs=(P(None, "gx", "gy", "gz"), P("gx", "gy", "gz")),
        check_vma=False,
    )
```

```python
import functools
import jax
import jax.numpy as jnp
from jax import lax
from jax.experimental import pallas as pl
from jax.experimental.pallas import tpu as pltpu
from jax.sharding import PartitionSpec as P

LOW_BOUND = 0.2
HIGH_BOUND = 1.8
OMEGA = 2.0 / 3.0
THETA = (HIGH_BOUND + LOW_BOUND) / 2.0
DELTA = (HIGH_BOUND - LOW_BOUND) / 2.0
SIGMA = THETA / DELTA
RHO_ZERO = 1.0 / SIGMA
RHO_ONE = 1.0 / (2.0 * SIGMA - RHO_ZERO)
WEIGHT = 2.0 * RHO_ONE / DELTA
KEEP = RHO_ONE * RHO_ZERO
GAIN = 1.0 + KEEP + WEIGHT * THETA

DEPTH = 3
COARSE_DEPTH = 2
EDGE = 4
OFFSETS = [
    (dx, dy, dz)
    for dx in (-1, 0, 1)
    for dy in (-1, 0, 1)
    for dz in (-1, 0, 1)
    if (dx, dy, dz) != (0, 0, 0)
]


def roll(x, shift, axis):
    return pltpu.roll(x, shift % x.shape[axis], axis)


def side(d):
    return 0 if d < 0 else 1


class Halo:
    def __init__(self, planes, comps, depth, refs):
        self.n, self.c, self.d = planes, comps, depth
        self.own, self.yp, self.zp, self.xb, self.yb, self.xyb, self.zb, self.ss, self.rs = refs

    @staticmethod
    def shapes(planes, comps, depth, rows, lanes):
        half = planes * comps // 2
        slots = -(-planes * comps * 2 * EDGE // lanes)
        f32 = jnp.float32
        return [
            pltpu.VMEM((planes, comps, rows, lanes), f32),
            pltpu.VMEM((2, half, rows, lanes), f32),
            pltpu.VMEM((slots, rows, lanes), f32),
            pltpu.VMEM((2, depth, comps, rows, lanes), f32),
            pltpu.VMEM((2, half, rows, lanes), f32),
            pltpu.VMEM((2, 2, depth * comps // 2, rows, lanes), f32),
            pltpu.VMEM((3, 3, 2, slots, rows, lanes), f32),
            pltpu.SemaphoreType.DMA((len(OFFSETS),)),
            pltpu.SemaphoreType.DMA((len(OFFSETS),)),
        ]

    def clear(self):
        for ref in (self.xb, self.yb, self.xyb, self.zb):
            ref[...] = jnp.zeros(ref.shape, ref.dtype)

    def pack(self):
        rows, lanes = self.own.shape[2:]
        row = lax.broadcasted_iota(jnp.int32, (rows, lanes), 0)
        slot = lax.broadcasted_iota(jnp.int32, (rows, lanes), 1) // (2 * EDGE)
        flat = [self.own[k, c] for k in range(self.n) for c in range(self.c)]
        for q in range(len(flat) // 2):
            even, odd = flat[2 * q], roll(flat[2 * q + 1], EDGE, 0)
            self.yp[0, q] = jnp.where(row < EDGE, even, odd)
            self.yp[1, q] = jnp.where(row < EDGE, odd, even)
        per = lanes // (2 * EDGE)
        for first in range(0, len(flat), per):
            strip = jnp.zeros((rows, lanes), jnp.float32)
            for s, v in enumerate(flat[first : first + per]):
                strip = jnp.where(slot == s, roll(v, s * 2 * EDGE + EDGE, 1), strip)
            self.zp[first // per] = strip

    def copy(self, index, me, receive):
        dx, dy, dz = OFFSETS[index]
        lo = 0 if dx < 0 else self.n - self.d
        half = self.d * self.c // 2
        rx, ry, rz = (dx, dy, dz) if receive else (-dx, -dy, -dz)
        if dz:
            src, dst = self.zp, self.zb.at[rx + 1, ry + 1, side(rz)]
        elif dx and dy:
            src = self.yp.at[side(dy), pl.ds(lo * self.c // 2, half)]
            dst = self.xyb.at[side(rx), side(ry)]
        elif dx:
            src, dst = self.own.at[pl.ds(lo, self.d)], self.xb.at[side(rx)]
        else:
            src, dst = self.yp.at[side(dy)], self.yb.at[side(ry)]
        arrival = index if receive else len(OFFSETS) - 1 - index
        return pltpu.make_async_remote_copy(
            src_ref=src,
            dst_ref=dst,
            send_sem=self.ss.at[index],
            recv_sem=self.rs.at[arrival],
            device_id=target(me, OFFSETS[index]),
            device_id_type=pl.DeviceIdType.MESH,
        )

    def send(self, me, exists):
        for index in ORDER:
            @pl.when(exists[index])
            def _():
                self.copy(index, me, False).start()

    def arrive(self, me, exists):
        for index in ORDER:
            @pl.when(exists[index])
            def _():
                self.copy(index, me, True).wait_recv()

    def drain(self, me, exists):
        for index in ORDER:
            @pl.when(exists[index])
            def _():
                self.copy(index, me, False).wait_send()

    def unpack(self, out):
        rows, lanes = self.own.shape[2:]
        row = lax.broadcasted_iota(jnp.int32, (rows, lanes), 0)
        lane = lax.broadcasted_iota(jnp.int32, (rows, lanes), 1)
        high = lane % (2 * EDGE) < EDGE
        per = lanes // (2 * EDGE)
        half = self.d * self.c // 2
        skip = (self.n - self.d) * self.c // 2
        for dx in (-1, 0, 1):
            strips = []
            for t in range(self.zp.shape[0]):
                at = [
                    jnp.where(high, self.zb[dx + 1, dy + 1, 0, t], self.zb[dx + 1, dy + 1, 1, t])
                    for dy in (-1, 0, 1)
                ]
                strips.append((at[1], jnp.where(row < EDGE, at[2], at[0])))
            first = self.n - self.d if dx < 0 else 0
            last = self.d if dx > 0 else self.n
            for k in range(first, last):
                p = k + self.d + dx * self.n
                for c in range(self.c):
                    idx = k * self.c + c
                    q = idx // 2
                    if dx == 0:
                        main, minus, plus = self.own[k, c], self.yb[0, q], self.yb[1, q]
                    else:
                        s = side(dx)
                        b = skip if dx < 0 else 0
                        main = self.xb[s, k - first, c]
                        minus, plus = self.xyb[s, 0, q - b], self.xyb[s, 1, q - b]
                    if idx % 2 == 0:
                        beside = jnp.where(row < EDGE, plus, minus)
                    else:
                        beside = roll(jnp.where(row < EDGE, minus, plus), EDGE, 0)
                    back = -((idx % per) * 2 * EDGE + EDGE)
                    mid, far = strips[idx // per]
                    out[p, c, :rows, :lanes] = main
                    out[p, c, :rows, lanes:] = roll(mid, back, 1)
                    out[p, c, rows:, :lanes] = beside
                    out[p, c, rows:, lanes:] = roll(far, back, 1)


ORDER = sorted(range(len(OFFSETS)), key=lambda i: -sum(abs(d) for d in OFFSETS[i]))


def target(me, offset):
    return {axis: at + d for (axis, at), d in zip(me.items(), offset)}


def coupling(st, rows, step):
    parts = 3 * rows
    width = 9 * parts
    padded = -(-width // 128) * 128
    row = lax.broadcasted_iota(jnp.int32, (rows, padded), 0)
    lane = lax.broadcasted_iota(jnp.int32, (rows, padded), 1)
    head = lax.broadcasted_iota(jnp.int32, (8, padded), 1)
    pair = (head // (3 * parts)) * 3 + (head % parts) // rows
    low = (lane % (3 * parts)) // parts == 2
    moved = (lane % rows - row + rows) % rows
    bands = [moved == (step * (b - 1)) % rows for b in range(3)]
    blocks = []
    for c in range(3):
        for i in range(3):
            block = jnp.zeros((rows, padded), jnp.float32)
            for b in range(3):
                line = jnp.zeros((8, padded), jnp.float32)
                for a in range(3):
                    for j in range(3):
                        line = jnp.where(pair == a * 3 + j, st[i, j, a * 9 + b * 3 + c], line)
                block = jnp.where(bands[b], jnp.tile(line, (rows // 8, 1)), block)
            high = block.astype(jnp.bfloat16).astype(jnp.float32)
            blocks.append(jnp.where(low, block - high, high))
    return blocks


def put(parts, p, j, v):
    rows = v.shape[0]
    high = v.astype(jnp.bfloat16)
    low = (v - high.astype(jnp.float32)).astype(jnp.bfloat16)
    parts[p, 0, j] = high
    parts[p, 1, j] = low
    parts[p, 2, j] = high


def product(matrix, parts, p):
    depth = 3 * 9 * parts.shape[3]
    window = parts[pl.ds(p - 1, 3)].reshape(depth, parts.shape[4])
    return jnp.dot(matrix[:, :depth], window, preferred_element_type=jnp.float32)


def stencil(matrix, parts, p, rows, step):
    lanes = parts.shape[4]
    r = product(matrix, parts, p)
    at = lambda c, i: r[(c * 3 + i) * rows : (c * 3 + i + 1) * rows]
    return [at(1, i) + roll(at(0, i), step, 1) + roll(at(2, i), lanes - step, 1) for i in range(3)]


def kernel(sizes, rv_in, rp_in, ids_in, table, st, vout, pout, *scratch):
    planes, rows, lanes = ids_in.shape
    fine = Halo(planes, 4, DEPTH, scratch[:9])
    coarse = Halo(planes // 2, 3, COARSE_DEPTH, scratch[9:18])
    wide, smooth, cwide, middle, press, eta_ref = scratch[18:24]
    wide_p, smooth_p, cwide_p, middle_p, m_wide, m_own, m_coarse = scratch[24:31]
    rv, rp, ids, in_sem = scratch[31:]
    tall = 2 * rows
    me = {axis: lax.axis_index(axis) for axis in sizes}
    exists = []
    for offset in OFFSETS:
        ok = None
        for (axis, at), d in zip(me.items(), offset):
            if d:
                one = at > 0 if d < 0 else at < sizes[axis] - 1
                ok = one if ok is None else jnp.logical_and(ok, one)
        exists.append(ok)

    fine.clear()
    coarse.clear()
    barrier = pltpu.get_barrier_semaphore()
    for index in ORDER:
        @pl.when(exists[index])
        def _():
            pl.semaphore_signal(
                barrier,
                inc=1,
                device_id=target(me, OFFSETS[index]),
                device_id_type=pl.DeviceIdType.MESH,
            )

    loads = [
        pltpu.make_async_copy(source, held, in_sem.at[n])
        for n, (source, held) in enumerate(((rv_in, rv), (rp_in, rp), (ids_in, ids)))
    ]
    for load in loads:
        load.start()
    blocks = coupling(st, tall, 1)
    m_wide[...] = jnp.concatenate(blocks, axis=0).astype(jnp.bfloat16)
    m_own[...] = jnp.concatenate([b[:rows] for b in blocks], axis=0).astype(jnp.bfloat16)

    kc = jnp.full((rows, lanes), (st[0, 0, 13] + st[1, 1, 13] + st[2, 2, 13]) / 3.0, jnp.float32)
    inv_kc = 1.0 / kc
    inv_wide = jnp.tile(inv_kc, (2, 2))
    for load in loads:
        load.wait()
    for k in range(planes):
        eta = jnp.zeros((rows, lanes), jnp.float32)
        for layer in range(table.shape[0]):
            eta = jnp.where(ids[k] == layer, table[layer], eta)
        eta_ref[k] = eta
        dinv = 1.0 / (eta * kc)
        for i in range(3):
            fine.own[k, i] = dinv * rv[i, k] / THETA
        fine.own[k, 3] = (OMEGA / 6.0) * eta * rp[k]
    fine.pack()
    peers = 1
    for axis, at in me.items():
        peers = peers * (
            1 + (at > 0).astype(jnp.int32) + (at < sizes[axis] - 1).astype(jnp.int32)
        )
    pl.semaphore_wait(barrier, peers - 1)
    fine.send(me, exists)
    m_coarse[...] = jnp.concatenate(coupling(st, tall, 2), axis=0).astype(jnp.bfloat16)

    row = lax.broadcasted_iota(jnp.int32, (2 * rows, 2 * lanes), 0)
    lane = lax.broadcasted_iota(jnp.int32, (2 * rows, 2 * lanes), 1)
    gx, gy, gz = sizes
    has_low = {axis: (me[axis] > 0).astype(jnp.float32) for axis in sizes}
    has_high = {axis: (me[axis] < sizes[axis] - 1).astype(jnp.float32) for axis in sizes}
    mask = jnp.where(row < rows, 1.0, jnp.where(row < rows + EDGE, has_high[gy], has_low[gy]))
    mask = mask * jnp.where(
        lane < lanes, 1.0, jnp.where(lane < lanes + lanes // 2, has_high[gz], has_low[gz])
    )

    def plane_mask(x):
        inside = jnp.where(x < 0, has_low[gx], jnp.where(x >= planes, has_high[gx], 1.0))
        return mask * inside

    fine.arrive(me, exists)
    fine.unpack(wide)
    for p in range(planes + 2 * DEPTH):
        for j in range(3):
            put(wide_p, p, j, wide[p, j])

    def smoothing(x):
        m = plane_mask(x)
        sums = stencil(m_wide, wide_p, x + DEPTH, tall, 1)
        for i in range(3):
            value = (GAIN * wide[x + DEPTH, i] - (WEIGHT * inv_wide) * sums[i]) * m
            smooth[x + 2, i] = value
            put(smooth_p, x + 2, i, value)

    @pl.loop(-1, planes + 1)
    def _(x):
        smoothing(x)

    even_row = lax.broadcasted_iota(jnp.int32, (rows, lanes), 0) % 2 == 0
    even_lane = lax.broadcasted_iota(jnp.int32, (rows, lanes), 1) % 2 == 0

    def pair_sum(v):
        v = v + jnp.where(even_row, roll(v, rows - 1, 0), roll(v, 1, 0))
        return v + jnp.where(even_lane, roll(v, lanes - 1, 1), roll(v, 1, 1))

    @pl.loop(0, planes // 2)
    def _(h):
        parts = [None] * 3
        eta_sum = None
        for half in range(2):
            x = 2 * h + half
            eta = eta_ref[x]
            eta_sum = eta if eta_sum is None else eta_sum + eta
            sums = stencil(m_own, smooth_p, x + 2, rows, 1)
            for i in range(3):
                value = eta * ((kc * THETA) * fine.own[x, i] - sums[i][:, :lanes])
                parts[i] = value if parts[i] is None else parts[i] + value
        dinv_c = 4.0 / (pair_sum(eta_sum) * kc * THETA)
        for i in range(3):
            coarse.own[h, i] = dinv_c * pair_sum(parts[i])

    coarse.pack()
    coarse.send(me, exists)

    smoothing(-2)
    smoothing(planes + 1)

    def star(ref, x):
        v = ref(x)
        total = ref(x - 1) + ref(x + 1)
        total = total + roll(v, 1, 0) + roll(v, 2 * rows - 1, 0)
        return total + roll(v, 1, 1) + roll(v, 2 * lanes - 1, 1)

    @pl.loop(-1, planes + 1)
    def _(x):
        near = star(lambda k: wide[k + DEPTH, 3], x)
        press[x + 1] = ((2.0 - OMEGA) * wide[x + DEPTH, 3] + (OMEGA / 6.0) * near) * plane_mask(x)

    @pl.loop(0, planes)
    def _(x):
        near = star(lambda k: press[k + 1], x)
        value = wide[x + DEPTH, 3] + (1.0 - OMEGA) * press[x + 1] + (OMEGA / 6.0) * near
        pout[x] = value[:rows, :lanes]

    coarse.arrive(me, exists)
    coarse.unpack(cwide)
    for p in range(planes // 2 + 2 * COARSE_DEPTH):
        for j in range(3):
            put(cwide_p, p, j, cwide[p, j])

    @pl.loop(-1, planes // 2 + 1)
    def _(h):
        sums = stencil(m_coarse, cwide_p, h + COARSE_DEPTH, tall, 2)
        m = plane_mask(2 * h)
        for i in range(3):
            value = GAIN * cwide[h + COARSE_DEPTH, i] - (WEIGHT * inv_wide) * sums[i]
            value = value * m
            for half in range(2):
                start = smooth[2 * h + 2 + half, i] + value
                smooth[2 * h + 2 + half, i] = start
                put(smooth_p, 2 * h + 2 + half, i, start)

    @pl.loop(-1, planes + 1)
    def _(x):
        m = plane_mask(x)
        sums = stencil(m_wide, smooth_p, x + 2, tall, 1)
        for i in range(3):
            first = wide[x + DEPTH, i] - (inv_wide / THETA) * sums[i]
            value = smooth[x + 2, i] + first * m
            middle[x + 1, i] = value[:rows, :lanes]
            put(middle_p, x + 1, i, value)

    @pl.loop(0, planes)
    def _(x):
        sums = stencil(m_own, middle_p, x + 1, rows, 1)
        for i in range(3):
            mid = middle[x + 1, i]
            first = mid - smooth[x + 2, i, :rows, :lanes]
            scaled = (WEIGHT * THETA) * fine.own[x, i] - (WEIGHT * inv_kc) * sums[i][:, :lanes]
            vout[i, x] = mid + KEEP * first + scaled

    fine.drain(me, exists)
    coarse.drain(me, exists)


def write_out(v, p, vout, pout, sem):
    first = pltpu.make_async_copy(v, vout, sem.at[0])
    second = pltpu.make_async_copy(p, pout, sem.at[1])
    first.start()
    second.start()
    first.wait()
    second.wait()


def on_device(sizes, rhs_velocity, rhs_pressure, layer_ids, visc_table, stencil):
    planes, rows, lanes = layer_ids.shape
    f32 = jnp.float32
    columns = -(-54 * rows // 128) * 128
    vmem = pl.BlockSpec(memory_space=pltpu.VMEM)
    hbm = pl.BlockSpec(memory_space=pl.ANY)
    smem = pl.BlockSpec(memory_space=pltpu.SMEM)
    results = pl.pallas_call(
        functools.partial(kernel, sizes),
        out_shape=(
            pltpu.VMEM(rhs_velocity.shape, f32),
            pltpu.VMEM(rhs_pressure.shape, f32),
        ),
        in_specs=[hbm, hbm, hbm, smem, smem],
        out_specs=(vmem, vmem),
        scratch_shapes=[
            *Halo.shapes(planes, 4, DEPTH, rows, lanes),
            *Halo.shapes(planes // 2, 3, COARSE_DEPTH, rows, lanes),
            pltpu.VMEM((planes + 2 * DEPTH, 4, 2 * rows, 2 * lanes), f32),
            pltpu.VMEM((planes + 4, 3, 2 * rows, 2 * lanes), f32),
            pltpu.VMEM((planes // 2 + 2 * COARSE_DEPTH, 3, 2 * rows, 2 * lanes), f32),
            pltpu.VMEM((planes + 2, 3, rows, lanes), f32),
            pltpu.VMEM((planes + 2, 2 * rows, 2 * lanes), f32),
            pltpu.VMEM((planes, rows, lanes), f32),
            *(
                pltpu.VMEM((count, 3, 3, 2 * rows, 2 * lanes), jnp.bfloat16)
                for count in (
                    planes + 2 * DEPTH,
                    planes + 4,
                    planes // 2 + 2 * COARSE_DEPTH,
                    planes + 2,
                )
            ),
            pltpu.VMEM((18 * rows, columns), jnp.bfloat16),
            pltpu.VMEM((9 * rows, columns), jnp.bfloat16),
            pltpu.VMEM((18 * rows, columns), jnp.bfloat16),
            pltpu.VMEM(rhs_velocity.shape, f32),
            pltpu.VMEM(rhs_pressure.shape, f32),
            pltpu.VMEM(layer_ids.shape, layer_ids.dtype),
            pltpu.SemaphoreType.DMA((3,)),
        ],
        compiler_params=pltpu.CompilerParams(collective_id=0, has_side_effects=True),
        name="stokes",
    )(rhs_velocity, rhs_pressure, layer_ids, visc_table, jnp.transpose(stencil, (1, 2, 0)))
    return pl.pallas_call(
        write_out,
        out_shape=tuple(jax.ShapeDtypeStruct(r.shape, f32) for r in results),
        in_specs=[hbm, hbm],
        out_specs=(hbm, hbm),
        scratch_shapes=[pltpu.SemaphoreType.DMA((2,))],
        compiler_params=pltpu.CompilerParams(vmem_limit_bytes=1 << 20),
        name="write_out",
    )(*results)


def solution(mesh):
    placed = (P(None, "gx", "gy", "gz"), P("gx", "gy", "gz"), P("gx", "gy", "gz"), P(), P())
    sizes = {axis: mesh.shape[axis] for axis in ("gx", "gy", "gz")}
    return jax.shard_map(
        functools.partial(on_device, sizes),
        mesh=mesh,
        in_specs=placed,
        out_specs=(P(None, "gx", "gy", "gz"), P("gx", "gy", "gz")),
        check_vma=False,
    )
```

```python
import functools
import jax
import jax.numpy as jnp
from jax import lax
from jax.experimental import pallas as pl
from jax.experimental.pallas import tpu as pltpu
from jax.sharding import PartitionSpec as P

LOW_BOUND = 0.2
HIGH_BOUND = 1.8
OMEGA = 2.0 / 3.0
THETA = (HIGH_BOUND + LOW_BOUND) / 2.0
DELTA = (HIGH_BOUND - LOW_BOUND) / 2.0
SIGMA = THETA / DELTA
RHO_ZERO = 1.0 / SIGMA
RHO_ONE = 1.0 / (2.0 * SIGMA - RHO_ZERO)
WEIGHT = 2.0 * RHO_ONE / DELTA
KEEP = RHO_ONE * RHO_ZERO
GAIN = 1.0 + KEEP + WEIGHT * THETA

DEPTH = 3
COARSE_DEPTH = 2
EDGE = 4
OFFSETS = [
    (dx, dy, dz)
    for dx in (-1, 0, 1)
    for dy in (-1, 0, 1)
    for dz in (-1, 0, 1)
    if (dx, dy, dz) != (0, 0, 0)
]


def roll(x, shift, axis):
    return pltpu.roll(x, shift % x.shape[axis], axis)


def side(d):
    return 0 if d < 0 else 1


class Halo:
    def __init__(self, planes, comps, depth, refs):
        self.n, self.c, self.d = planes, comps, depth
        self.own, self.yp, self.zp, self.xb, self.yb, self.xyb, self.zb, self.ss, self.rs = refs

    @staticmethod
    def shapes(planes, comps, depth, rows, lanes):
        half = planes * comps // 2
        slots = -(-planes * comps * 2 * EDGE // lanes)
        f32 = jnp.float32
        return [
            pltpu.VMEM((planes, comps, rows, lanes), f32),
            pltpu.VMEM((2, half, rows, lanes), f32),
            pltpu.VMEM((slots, rows, lanes), f32),
            pltpu.VMEM((2, depth, comps, rows, lanes), f32),
            pltpu.VMEM((2, half, rows, lanes), f32),
            pltpu.VMEM((2, 2, depth * comps // 2, rows, lanes), f32),
            pltpu.VMEM((3, 3, 2, slots, rows, lanes), f32),
            pltpu.SemaphoreType.DMA((len(OFFSETS),)),
            pltpu.SemaphoreType.DMA((len(OFFSETS),)),
        ]

    def clear(self):
        for ref in (self.xb, self.yb, self.xyb, self.zb):
            ref[...] = jnp.zeros(ref.shape, ref.dtype)

    def pack(self):
        rows, lanes = self.own.shape[2:]
        row = lax.broadcasted_iota(jnp.int32, (rows, lanes), 0)
        slot = lax.broadcasted_iota(jnp.int32, (rows, lanes), 1) // (2 * EDGE)
        flat = [self.own[k, c] for k in range(self.n) for c in range(self.c)]
        for q in range(len(flat) // 2):
            even, odd = flat[2 * q], roll(flat[2 * q + 1], EDGE, 0)
            self.yp[0, q] = jnp.where(row < EDGE, even, odd)
            self.yp[1, q] = jnp.where(row < EDGE, odd, even)
        per = lanes // (2 * EDGE)
        for first in range(0, len(flat), per):
            strip = jnp.zeros((rows, lanes), jnp.float32)
            for s, v in enumerate(flat[first : first + per]):
                strip = jnp.where(slot == s, roll(v, s * 2 * EDGE + EDGE, 1), strip)
            self.zp[first // per] = strip

    def copy(self, index, me, receive):
        dx, dy, dz = OFFSETS[index]
        lo = 0 if dx < 0 else self.n - self.d
        half = self.d * self.c // 2
        rx, ry, rz = (dx, dy, dz) if receive else (-dx, -dy, -dz)
        if dz:
            src, dst = self.zp, self.zb.at[rx + 1, ry + 1, side(rz)]
        elif dx and dy:
            src = self.yp.at[side(dy), pl.ds(lo * self.c // 2, half)]
            dst = self.xyb.at[side(rx), side(ry)]
        elif dx:
            src, dst = self.own.at[pl.ds(lo, self.d)], self.xb.at[side(rx)]
        else:
            src, dst = self.yp.at[side(dy)], self.yb.at[side(ry)]
        arrival = index if receive else len(OFFSETS) - 1 - index
        return pltpu.make_async_remote_copy(
            src_ref=src,
            dst_ref=dst,
            send_sem=self.ss.at[index],
            recv_sem=self.rs.at[arrival],
            device_id=target(me, OFFSETS[index]),
            device_id_type=pl.DeviceIdType.MESH,
        )

    def send(self, me, exists):
        for index in ORDER:
            @pl.when(exists[index])
            def _():
                self.copy(index, me, False).start()

    def arrive(self, me, exists):
        for index in ORDER:
            @pl.when(exists[index])
            def _():
                self.copy(index, me, True).wait_recv()

    def drain(self, me, exists):
        for index in ORDER:
            @pl.when(exists[index])
            def _():
                self.copy(index, me, False).wait_send()

    def unpack(self, out):
        rows, lanes = self.own.shape[2:]
        row = lax.broadcasted_iota(jnp.int32, (rows, lanes), 0)
        lane = lax.broadcasted_iota(jnp.int32, (rows, lanes), 1)
        high = lane % (2 * EDGE) < EDGE
        per = lanes // (2 * EDGE)
        half = self.d * self.c // 2
        skip = (self.n - self.d) * self.c // 2
        for dx in (-1, 0, 1):
            strips = []
            for t in range(self.zp.shape[0]):
                at = [
                    jnp.where(high, self.zb[dx + 1, dy + 1, 0, t], self.zb[dx + 1, dy + 1, 1, t])
                    for dy in (-1, 0, 1)
                ]
                strips.append((at[1], jnp.where(row < EDGE, at[2], at[0])))
            first = self.n - self.d if dx < 0 else 0
            last = self.d if dx > 0 else self.n
            for k in range(first, last):
                p = k + self.d + dx * self.n
                for c in range(self.c):
                    idx = k * self.c + c
                    q = idx // 2
                    if dx == 0:
                        main, minus, plus = self.own[k, c], self.yb[0, q], self.yb[1, q]
                    else:
                        s = side(dx)
                        b = skip if dx < 0 else 0
                        main = self.xb[s, k - first, c]
                        minus, plus = self.xyb[s, 0, q - b], self.xyb[s, 1, q - b]
                    if idx % 2 == 0:
                        beside = jnp.where(row < EDGE, plus, minus)
                    else:
                        beside = roll(jnp.where(row < EDGE, minus, plus), EDGE, 0)
                    back = -((idx % per) * 2 * EDGE + EDGE)
                    mid, far = strips[idx // per]
                    out[p, c, :rows, :lanes] = main
                    out[p, c, :rows, lanes:] = roll(mid, back, 1)
                    out[p, c, rows:, :lanes] = beside
                    out[p, c, rows:, lanes:] = roll(far, back, 1)


ORDER = sorted(range(len(OFFSETS)), key=lambda i: -sum(abs(d) for d in OFFSETS[i]))


def target(me, offset):
    return {axis: at + d for (axis, at), d in zip(me.items(), offset)}


def coupling(st, rows, step):
    parts = 3 * rows
    width = 9 * parts
    padded = -(-width // 128) * 128
    row = lax.broadcasted_iota(jnp.int32, (rows, padded), 0)
    lane = lax.broadcasted_iota(jnp.int32, (rows, padded), 1)
    head = lax.broadcasted_iota(jnp.int32, (8, padded), 1)
    pair = (head // (3 * parts)) * 3 + (head % parts) // rows
    low = (lane % (3 * parts)) // parts == 2
    moved = (lane % rows - row + rows) % rows
    bands = [moved == (step * (b - 1)) % rows for b in range(3)]
    blocks = []
    for c in range(3):
        for i in range(3):
            block = jnp.zeros((rows, padded), jnp.float32)
            for b in range(3):
                line = jnp.zeros((8, padded), jnp.float32)
                for a in range(3):
                    for j in range(3):
                        line = jnp.where(pair == a * 3 + j, st[i, j, a * 9 + b * 3 + c], line)
                block = jnp.where(bands[b], jnp.tile(line, (rows // 8, 1)), block)
            high = block.astype(jnp.bfloat16).astype(jnp.float32)
            blocks.append(jnp.where(low, block - high, high))
    return blocks


def put(parts, p, j, v):
    rows = v.shape[0]
    high = v.astype(jnp.bfloat16)
    low = (v - high.astype(jnp.float32)).astype(jnp.bfloat16)
    parts[p, 0, j] = high
    parts[p, 1, j] = low
    parts[p, 2, j] = high


def product(matrix, parts, p):
    depth = 3 * 9 * parts.shape[3]
    window = parts[pl.ds(p - 1, 3)].reshape(depth, parts.shape[4])
    return jnp.dot(matrix[:, :depth], window, preferred_element_type=jnp.float32)


def stencil(matrix, parts, p, rows, step):
    lanes = parts.shape[4]
    r = product(matrix, parts, p)
    at = lambda c, i: r[(c * 3 + i) * rows : (c * 3 + i + 1) * rows]
    return [at(1, i) + roll(at(0, i), step, 1) + roll(at(2, i), lanes - step, 1) for i in range(3)]


def kernel(sizes, rv_in, rp_in, ids_in, table, st, vout, pout, *scratch):
    planes, rows, lanes = ids_in.shape
    fine = Halo(planes, 4, DEPTH, scratch[:9])
    coarse = Halo(planes // 2, 3, COARSE_DEPTH, scratch[9:18])
    wide, smooth, cwide, middle, press, eta_ref = scratch[18:24]
    wide_p, smooth_p, cwide_p, middle_p, m_wide, m_own, m_coarse = scratch[24:31]
    rv, rp, ids, in_sem = scratch[31:]
    tall = 2 * rows
    me = {axis: lax.axis_index(axis) for axis in sizes}
    exists = []
    for offset in OFFSETS:
        ok = None
        for (axis, at), d in zip(me.items(), offset):
            if d:
                one = at > 0 if d < 0 else at < sizes[axis] - 1
                ok = one if ok is None else jnp.logical_and(ok, one)
        exists.append(ok)

    fine.clear()
    coarse.clear()
    barrier = pltpu.get_barrier_semaphore()
    for index in ORDER:
        @pl.when(exists[index])
        def _():
            pl.semaphore_signal(
                barrier,
                inc=1,
                device_id=target(me, OFFSETS[index]),
                device_id_type=pl.DeviceIdType.MESH,
            )

    loads = [
        pltpu.make_async_copy(source, held, in_sem.at[n])
        for n, (source, held) in enumerate(((rv_in, rv), (rp_in, rp), (ids_in, ids)))
    ]
    for load in loads:
        load.start()
    blocks = coupling(st, tall, 1)
    m_wide[...] = jnp.concatenate(blocks, axis=0).astype(jnp.bfloat16)
    m_own[...] = jnp.concatenate([b[:rows] for b in blocks], axis=0).astype(jnp.bfloat16)

    kc = jnp.full((rows, lanes), (st[0, 0, 13] + st[1, 1, 13] + st[2, 2, 13]) / 3.0, jnp.float32)
    inv_kc = 1.0 / kc
    inv_wide = jnp.tile(inv_kc, (2, 2))
    for load in loads:
        load.wait()
    for k in range(planes):
        eta = jnp.zeros((rows, lanes), jnp.float32)
        for layer in range(table.shape[0]):
            eta = jnp.where(ids[k] == layer, table[layer], eta)
        eta_ref[k] = eta
        dinv = 1.0 / (eta * kc)
        for i in range(3):
            fine.own[k, i] = dinv * rv[i, k] / THETA
        fine.own[k, 3] = (OMEGA / 6.0) * eta * rp[k]
    fine.pack()
    peers = 1
    for axis, at in me.items():
        peers = peers * (
            1 + (at > 0).astype(jnp.int32) + (at < sizes[axis] - 1).astype(jnp.int32)
        )
    pl.semaphore_wait(barrier, peers - 1)
    fine.send(me, exists)
    m_coarse[...] = jnp.concatenate(coupling(st, tall, 2), axis=0).astype(jnp.bfloat16)

    row = lax.broadcasted_iota(jnp.int32, (2 * rows, 2 * lanes), 0)
    lane = lax.broadcasted_iota(jnp.int32, (2 * rows, 2 * lanes), 1)
    gx, gy, gz = sizes
    has_low = {axis: (me[axis] > 0).astype(jnp.float32) for axis in sizes}
    has_high = {axis: (me[axis] < sizes[axis] - 1).astype(jnp.float32) for axis in sizes}
    mask = jnp.where(row < rows, 1.0, jnp.where(row < rows + EDGE, has_high[gy], has_low[gy]))
    mask = mask * jnp.where(
        lane < lanes, 1.0, jnp.where(lane < lanes + lanes // 2, has_high[gz], has_low[gz])
    )

    def plane_mask(x):
        inside = jnp.where(x < 0, has_low[gx], jnp.where(x >= planes, has_high[gx], 1.0))
        return mask * inside

    fine.arrive(me, exists)
    fine.unpack(wide)
    for p in range(planes + 2 * DEPTH):
        for j in range(3):
            put(wide_p, p, j, wide[p, j])

    def smoothing(x):
        m = plane_mask(x)
        sums = stencil(m_wide, wide_p, x + DEPTH, tall, 1)
        for i in range(3):
            value = (GAIN * wide[x + DEPTH, i] - (WEIGHT * inv_wide) * sums[i]) * m
            smooth[x + 2, i] = value
            put(smooth_p, x + 2, i, value)

    @pl.loop(-1, planes + 1, unroll=True)
    def _(x):
        smoothing(x)

    even_row = lax.broadcasted_iota(jnp.int32, (rows, lanes), 0) % 2 == 0
    even_lane = lax.broadcasted_iota(jnp.int32, (rows, lanes), 1) % 2 == 0

    def pair_sum(v):
        v = v + jnp.where(even_row, roll(v, rows - 1, 0), roll(v, 1, 0))
        return v + jnp.where(even_lane, roll(v, lanes - 1, 1), roll(v, 1, 1))

    @pl.loop(0, planes // 2, unroll=True)
    def _(h):
        parts = [None] * 3
        eta_sum = None
        for half in range(2):
            x = 2 * h + half
            eta = eta_ref[x]
            eta_sum = eta if eta_sum is None else eta_sum + eta
            sums = stencil(m_own, smooth_p, x + 2, rows, 1)
            for i in range(3):
                value = eta * ((kc * THETA) * fine.own[x, i] - sums[i][:, :lanes])
                parts[i] = value if parts[i] is None else parts[i] + value
        dinv_c = 4.0 / (pair_sum(eta_sum) * kc * THETA)
        for i in range(3):
            coarse.own[h, i] = dinv_c * pair_sum(parts[i])

    coarse.pack()
    coarse.send(me, exists)

    smoothing(-2)
    smoothing(planes + 1)

    def star(ref, x):
        v = ref(x)
        total = ref(x - 1) + ref(x + 1)
        total = total + roll(v, 1, 0) + roll(v, 2 * rows - 1, 0)
        return total + roll(v, 1, 1) + roll(v, 2 * lanes - 1, 1)

    @pl.loop(-1, planes + 1, unroll=True)
    def _(x):
        near = star(lambda k: wide[k + DEPTH, 3], x)
        press[x + 1] = ((2.0 - OMEGA) * wide[x + DEPTH, 3] + (OMEGA / 6.0) * near) * plane_mask(x)

    @pl.loop(0, planes, unroll=True)
    def _(x):
        near = star(lambda k: press[k + 1], x)
        value = wide[x + DEPTH, 3] + (1.0 - OMEGA) * press[x + 1] + (OMEGA / 6.0) * near
        pout[x] = value[:rows, :lanes]

    coarse.arrive(me, exists)
    coarse.unpack(cwide)
    for p in range(planes // 2 + 2 * COARSE_DEPTH):
        for j in range(3):
            put(cwide_p, p, j, cwide[p, j])

    @pl.loop(-1, planes // 2 + 1, unroll=True)
    def _(h):
        sums = stencil(m_coarse, cwide_p, h + COARSE_DEPTH, tall, 2)
        m = plane_mask(2 * h)
        for i in range(3):
            value = GAIN * cwide[h + COARSE_DEPTH, i] - (WEIGHT * inv_wide) * sums[i]
            value = value * m
            for half in range(2):
                start = smooth[2 * h + 2 + half, i] + value
                smooth[2 * h + 2 + half, i] = start
                put(smooth_p, 2 * h + 2 + half, i, start)

    @pl.loop(-1, planes + 1, unroll=True)
    def _(x):
        m = plane_mask(x)
        sums = stencil(m_wide, smooth_p, x + 2, tall, 1)
        for i in range(3):
            first = wide[x + DEPTH, i] - (inv_wide / THETA) * sums[i]
            value = smooth[x + 2, i] + first * m
            middle[x + 1, i] = value[:rows, :lanes]
            put(middle_p, x + 1, i, value)

    @pl.loop(0, planes, unroll=True)
    def _(x):
        sums = stencil(m_own, middle_p, x + 1, rows, 1)
        for i in range(3):
            mid = middle[x + 1, i]
            first = mid - smooth[x + 2, i, :rows, :lanes]
            scaled = (WEIGHT * THETA) * fine.own[x, i] - (WEIGHT * inv_kc) * sums[i][:, :lanes]
            vout[i, x] = mid + KEEP * first + scaled

    fine.drain(me, exists)
    coarse.drain(me, exists)


def write_out(v, p, vout, pout, sem):
    first = pltpu.make_async_copy(v, vout, sem.at[0])
    second = pltpu.make_async_copy(p, pout, sem.at[1])
    first.start()
    second.start()
    first.wait()
    second.wait()


def on_device(sizes, rhs_velocity, rhs_pressure, layer_ids, visc_table, stencil):
    planes, rows, lanes = layer_ids.shape
    f32 = jnp.float32
    columns = -(-54 * rows // 128) * 128
    vmem = pl.BlockSpec(memory_space=pltpu.VMEM)
    hbm = pl.BlockSpec(memory_space=pl.ANY)
    smem = pl.BlockSpec(memory_space=pltpu.SMEM)
    results = pl.pallas_call(
        functools.partial(kernel, sizes),
        out_shape=(
            pltpu.VMEM(rhs_velocity.shape, f32),
            pltpu.VMEM(rhs_pressure.shape, f32),
        ),
        in_specs=[hbm, hbm, hbm, smem, smem],
        out_specs=(vmem, vmem),
        scratch_shapes=[
            *Halo.shapes(planes, 4, DEPTH, rows, lanes),
            *Halo.shapes(planes // 2, 3, COARSE_DEPTH, rows, lanes),
            pltpu.VMEM((planes + 2 * DEPTH, 4, 2 * rows, 2 * lanes), f32),
            pltpu.VMEM((planes + 4, 3, 2 * rows, 2 * lanes), f32),
            pltpu.VMEM((planes // 2 + 2 * COARSE_DEPTH, 3, 2 * rows, 2 * lanes), f32),
            pltpu.VMEM((planes + 2, 3, rows, lanes), f32),
            pltpu.VMEM((planes + 2, 2 * rows, 2 * lanes), f32),
            pltpu.VMEM((planes, rows, lanes), f32),
            *(
                pltpu.VMEM((count, 3, 3, 2 * rows, 2 * lanes), jnp.bfloat16)
                for count in (
                    planes + 2 * DEPTH,
                    planes + 4,
                    planes // 2 + 2 * COARSE_DEPTH,
                    planes + 2,
                )
            ),
            pltpu.VMEM((18 * rows, columns), jnp.bfloat16),
            pltpu.VMEM((9 * rows, columns), jnp.bfloat16),
            pltpu.VMEM((18 * rows, columns), jnp.bfloat16),
            pltpu.VMEM(rhs_velocity.shape, f32),
            pltpu.VMEM(rhs_pressure.shape, f32),
            pltpu.VMEM(layer_ids.shape, layer_ids.dtype),
            pltpu.SemaphoreType.DMA((3,)),
        ],
        compiler_params=pltpu.CompilerParams(collective_id=0, has_side_effects=True),
        name="stokes",
    )(rhs_velocity, rhs_pressure, layer_ids, visc_table, jnp.transpose(stencil, (1, 2, 0)))
    return pl.pallas_call(
        write_out,
        out_shape=tuple(jax.ShapeDtypeStruct(r.shape, f32) for r in results),
        in_specs=[hbm, hbm],
        out_specs=(hbm, hbm),
        scratch_shapes=[pltpu.SemaphoreType.DMA((2,))],
        compiler_params=pltpu.CompilerParams(vmem_limit_bytes=1 << 20),
        name="write_out",
    )(*results)


def solution(mesh):
    placed = (P(None, "gx", "gy", "gz"), P("gx", "gy", "gz"), P("gx", "gy", "gz"), P(), P())
    sizes = {axis: mesh.shape[axis] for axis in ("gx", "gy", "gz")}
    return jax.shard_map(
        functools.partial(on_device, sizes),
        mesh=mesh,
        in_specs=placed,
        out_specs=(P(None, "gx", "gy", "gz"), P("gx", "gy", "gz")),
        check_vma=False,
    )
```
